128 devices in a mesh: kpt: 2 (over x_lo), grid: 64 (over x_hi, z, y, core).
Axes of the slice: x: 4 (x_hi: 2, x_lo: 2; x = x_hi * 2 + x_lo), y: 4, z: 4, core: 2. Of those that a mesh axis runs over, the one named last changes fastest.
Arguments:
- orbitals: bfloat16 [4, 2, 2, 512, 256, 256], P('kpt', None, None, 'grid'), may hold values from -6 to 6
- kweights: int32 [4], P('kpt'), may hold values from 1 to 16
- occupations: int32 [4, 2], P('kpt'), may hold values from 0 to 2
- z_basis: float32 [512, 512], replicated, may hold values from -0.25 to 0.25
- z_eigen: float32 [512], replicated, may hold values from 0.25 to 4
Outputs:
- potential: float32 [512, 256, 256], P('grid')
The draws below stay inside these ranges and needn't reach their ends.
All inputs are finite; a program needn't handle non-finite values.
Results may differ from the reference program's by a relative error of at most 0.0003.
Values sent between devices are 32-bit elements; how exact they have to be, the bound alone decides.
A program may use at most 64 MiB of HBM per device.

```python
import math
import jax
import jax.numpy as jnp
from jax import lax

NX = 256
NY = 256
NZ = 512
KPD = 2
BANDS = 2
KPOINTS = 4


def draw_kweights(key, part):
    first, second = jax.random.split(jax.random.fold_in(key, 11))
    base = jax.random.randint(first, (KPOINTS,), 1, 17)
    chosen = jax.random.randint(second, (), 0, KPOINTS)
    places = jnp.arange(KPOINTS, dtype=jnp.int32)
    return jnp.where(places == chosen, 16, base).astype(jnp.int32)


def draw_occupations(key, part):
    first, second = jax.random.split(jax.random.fold_in(key, 23))
    base = jax.random.randint(first, (KPOINTS * BANDS,), 0, 3)
    order = jax.random.permutation(second, KPOINTS * BANDS)
    mixed = jnp.where(order == 0, 0, jnp.where(order == 1, 2, base))
    return mixed.reshape(KPOINTS, BANDS).astype(jnp.int32)


def block_scale(own_key, extent, shards, low, top_value):
    def one(position, blocks):
        steps = jax.random.uniform(jax.random.fold_in(jax.random.fold_in(own_key, 6), position), (blocks,), jnp.float32, low / len(shards), top_value / len(shards))
        return jnp.repeat(jnp.exp(steps), extent[position] // blocks).reshape((-1,) + (1,) * (len(extent) - position - 1))

    loudness = one(*shards[0])
    for cut in shards[1:]:
        loudness = loudness * one(*cut)
    return loudness


def scatter_about(own_key, extent, scale, most, cuts=(), held_as=jnp.bfloat16):
    level = block_scale(own_key, extent, cuts, -0.22, 0.18) if cuts else 1.0
    values = jax.random.normal(own_key, extent, jnp.float32) * scale * level
    return jnp.minimum(jnp.maximum(values, -most), most).astype(held_as)


def setup_inputs(seed: int = 0) -> dict:
    keys = jax.random.split(jax.random.key(seed), 6)
    orbitals = scatter_about(keys[0], (KPOINTS, BANDS, 2, NZ, NX, NY), 1.0, 6.0, ((0, 2), (3, 64)))
    kweights = draw_kweights(jax.random.fold_in(keys[5], 71), 0)
    occupations = draw_occupations(jax.random.fold_in(keys[5], 71), 0)
    z_basis = scatter_about(keys[3], (NZ, NZ), NZ ** -0.5, 0.25, (), jnp.float32)
    z_eigen = jnp.clip(jnp.exp(jax.random.uniform(keys[4], (NZ,), jnp.float32, math.log(0.25), math.log(4.0))), 0.25, 4.0)
    return {"orbitals": orbitals, "kweights": kweights, "occupations": occupations, "z_basis": z_basis, "z_eigen": z_eigen}


precise = lax.Precision.HIGHEST


def reference(orbitals, kweights, occupations, z_basis, z_eigen):
    factor = (kweights[:, None] * occupations).astype(jnp.float32) / (16.0 * KPD * BANDS)

    def add_point(kpoint, running):
        values = lax.dynamic_index_in_dim(orbitals, kpoint, 0, keepdims=False).astype(jnp.float32)
        weights = lax.dynamic_index_in_dim(factor, kpoint, 0, keepdims=False)
        return running + jnp.sum(weights[:, None, None, None, None] * values * values, axis=(0, 1))

    density = lax.fori_loop(0, KPOINTS, add_point, jnp.zeros((NZ, NX, NY), jnp.float32))
    spectrum = jnp.fft.fft2(density, axes=(1, 2))
    stacked = jnp.stack([jnp.real(spectrum), jnp.imag(spectrum)]).astype(jnp.float32)
    wave_x = jnp.arange(NX).astype(jnp.float32)
    wave_y = jnp.arange(NY).astype(jnp.float32)
    shift_x = 2.0 * jnp.sin(jnp.pi * wave_x / NX)
    shift_y = 2.0 * jnp.sin(jnp.pi * wave_y / NY)
    shifted = shift_x[:, None] ** 2 + shift_y[None, :] ** 2
    factors = 1.0 / (z_eigen[:, None, None] + shifted[None])
    projected = jnp.einsum('zj,czab->cjab', z_basis, stacked, precision=precise)
    filtered = jnp.einsum('zj,cjab->czab', z_basis, projected * factors[None], precision=precise)
    potential = jnp.fft.ifft2(lax.complex(filtered[0], filtered[1]), axes=(1, 2))
    return jnp.real(potential).astype(jnp.float32)
```

```python
import functools

import jax
import jax.numpy as jnp
import numpy as np
from jax import lax
from jax.experimental import pallas as pl
from jax.experimental.pallas import tpu as pltpu
from jax.sharding import PartitionSpec as P

MESH = pl.DeviceIdType.MESH
f32 = jnp.float32
bf16 = jnp.bfloat16
N = 256
NZ = 512
LANES = 128
DEVICES = 128
PLANES = 8
QUAD = 4


def real_table():
    position = np.arange(N)
    angles = (position[:, None] * position[None, :] % N) * (2.0 * np.pi / N)
    return np.where(position[:, None] <= N // 2, np.cos(angles), np.sin(angles))


def tables():
    table = real_table()
    halves = []
    for one in (table.T, table):
        high = one.astype(bf16)
        low = (one - high.astype(np.float64)).astype(bf16)
        halves += [high, low]
    return np.stack(halves)


def mode_rows():
    position = np.arange(N)
    shift = (2.0 * np.sin(np.pi * position / N)) ** 2
    edges = (position == 0) | (position == N // 2)
    weight = np.where(edges, 1.0, 2.0) / N
    rows = np.zeros((8, N), np.float32)
    rows[0], rows[1] = shift, weight
    return rows


def split(value):
    high = value.astype(bf16)
    low = (value - high.astype(f32)).astype(bf16)
    return high, low


def dot(left, right):
    return jnp.dot(left, right, preferred_element_type=f32)


def dot3(left_high, left_low, right_high, right_low):
    return dot(left_high, right_high) + (dot(left_high, right_low) + dot(left_low, right_high))


def coords():
    k = lax.axis_index("kpt")
    g = lax.axis_index("grid")
    return g // 32 * 2 + k, lax.rem(g // 2, 4), lax.rem(g // 8, 4), lax.rem(g, 2)


def device(x, y, z, c):
    return lax.rem(x, 2), ((x // 2 * 4 + z) * 4 + y) * 2 + c


def peer(step):
    x, y, z, c = coords()
    mixed = lax.rem(step * 37, 128)
    return device(
        lax.rem(x + lax.rem(mixed, 4), 4),
        lax.rem(y + lax.rem(mixed // 4, 4), 4),
        lax.rem(z + lax.rem(mixed // 16, 4), 4),
        lax.rem(c + mixed // 64, 2),
    )


def rows_of(index, count):
    return pl.ds(pl.multiple_of(index * count, count), count)


def kernel(
    orb, kw, occ, zb, lam, tab_in, row_in, out,
    obuf, zbuf, lamv, tab, rowv, B, R, W, Q, Zh, Zl, ZhT, ZlT, fac,
    dh, dl, Xh, Xl, Yh, Yl, half,
    orb_sem, in_sem, send_sem, recv_sem, back_sem, got_sem, y_sem, z_sem, c_sem,
):
    k = lax.axis_index("kpt")
    g = lax.axis_index("grid")
    me = k * 64 + g
    x, y, z, c = coords()

    def along(axis, step):
        return device(
            lax.rem(x + step, 4) if axis == 0 else x,
            lax.rem(y + step, 4) if axis == 1 else y,
            lax.rem(z + step, 4) if axis == 2 else z,
            lax.rem(c + step, 2) if axis == 3 else c,
        )

    def signal(sem, axis):
        for step in range(1, 2 if axis == 3 else 4):
            tk, tg = along(axis, step)
            pl.semaphore_signal(sem, inc=1, device_id={"kpt": tk, "grid": tg}, device_id_type=MESH)

    barrier = pltpu.get_barrier_semaphore()
    for axis in range(4):
        signal(barrier, axis)

    def orb_copy(plane):
        return pltpu.make_async_copy(orb.at[:, :, :, plane], obuf.at[plane], orb_sem.at[plane])

    ins = [
        pltpu.make_async_copy(tab_in, tab, in_sem.at[0]),
        pltpu.make_async_copy(row_in, rowv, in_sem.at[1]),
        pltpu.make_async_copy(lam, lamv, in_sem.at[2]),
        pltpu.make_async_copy(zb, zbuf, in_sem.at[3]),
    ]
    orb_copy(0).start()
    ins[0].start()
    for plane in range(1, PLANES):
        orb_copy(plane).start()
    for one in ins[1:]:
        one.start()

    weight = [[(kw[p] * occ[p, b]).astype(f32) * (1.0 / 64.0) for b in range(2)] for p in range(2)]

    def plane_spectrum(plane):
        orb_copy(plane).wait()
        slot = plane % 2
        for r in range(0, N, 32):
            total = None
            for p in range(2):
                for b in range(2):
                    re = obuf[plane, p, b, 0, r : r + 32, :].astype(f32)
                    im = obuf[plane, p, b, 1, r : r + 32, :].astype(f32)
                    term = weight[p][b] * (re * re + im * im)
                    total = term if total is None else total + term
            high, low = split(total)
            dh[slot, r : r + 32, :] = high
            dl[slot, r : r + 32, :] = low
        along_y = dot3(dh[slot], dl[slot], tab[0], tab[1])
        high, low = split(along_y)
        both = dot3(tab[2], tab[3], high, low)
        h, q = plane // QUAD, plane % QUAD
        for e in range(2):
            for u in range(2):
                B[h, e, pl.ds(q * 2 + u, LANES, stride=8), :] = both[
                    e * LANES : (e + 1) * LANES, u * LANES : (u + 1) * LANES
                ]

    def send_out(h, e):
        def one(step, carry):
            tk, tg = peer(step)
            pltpu.make_async_remote_copy(
                src_ref=B.at[h, e, rows_of(tk * 64 + tg, 8)],
                dst_ref=R.at[e, rows_of(me * 2 + h, 8)],
                send_sem=send_sem,
                recv_sem=recv_sem.at[e],
                device_id={"kpt": tk, "grid": tg},
                device_id_type=MESH,
            ).start()
            return carry

        lax.fori_loop(1, DEVICES, one, 0)
        R[e, rows_of(me * 2 + h, 8), :] = B[h, e, rows_of(me, 8), :]

    plane_spectrum_after = []
    ins[0].wait()
    plane_spectrum(0)
    pl.semaphore_wait(barrier, 10)
    signal(y_sem, 1)
    plane_spectrum(1)
    pl.semaphore_wait(y_sem, 3)
    signal(z_sem, 2)
    plane_spectrum(2)
    pl.semaphore_wait(z_sem, 3)
    signal(c_sem, 3)
    plane_spectrum(3)
    pl.semaphore_wait(c_sem, 1)
    send_out(0, 0)
    for plane in range(QUAD, PLANES):
        plane_spectrum(plane)
    send_out(1, 0)
    send_out(0, 1)
    send_out(1, 1)

    for one in ins[1:]:
        one.wait()
    for r in range(0, NZ, LANES):
        rows = zbuf[r : r + LANES, :]
        high, low = split(rows)
        Zh[r : r + LANES, :] = high
        Zl[r : r + LANES, :] = low
        turned = rows.T
        high, low = split(turned)
        ZhT[:, r : r + LANES] = high
        ZlT[:, r : r + LANES] = low
    shift_y, weight_y = rowv[0:1, :], rowv[1:2, :]
    lanes = lax.broadcasted_iota(jnp.int32, (1, N), 1)
    for e in range(2):
        mine = lanes == e * LANES + me
        shift_x = jnp.sum(jnp.where(mine, shift_y, 0.0), axis=1, keepdims=True)
        weight_x = jnp.sum(jnp.where(mine, weight_y, 0.0), axis=1, keepdims=True)
        for r in range(0, NZ, LANES):
            column = jnp.broadcast_to(lamv[0:1, r : r + LANES], (LANES, LANES)).T
            for u in range(2):
                cols = slice(u * LANES, (u + 1) * LANES)
                fac[e, r : r + LANES, cols] = (weight_y[:, cols] * weight_x) / (
                    column + (shift_y[:, cols] + shift_x)
                )

    def solve(e):
        taken = R.at[e, pl.ds(0, (DEVICES - 1) * 16)]
        pltpu.make_async_copy(taken, taken, recv_sem.at[e]).wait()
        for u in range(2):
            cols = slice(u * LANES, (u + 1) * LANES)
            for r in range(0, NZ, LANES):
                first = R[e, pl.ds(r * 2 + u, LANES, stride=2), :]
                second = R[e, pl.ds(1024 + r * 2 + u, LANES, stride=2), :]
                high, low = split(first + second)
                Xh[r : r + LANES, cols] = high
                Xl[r : r + LANES, cols] = low
        for r in range(0, NZ, N):
            part = dot3(ZhT[r : r + N, :], ZlT[r : r + N, :], Xh[...], Xl[...])
            high, low = split(part * fac[e, r : r + N, :])
            Yh[r : r + N, :] = high
            Yl[r : r + N, :] = low
        for r in range(0, NZ, N):
            part = dot3(Zh[r : r + N, :], Zl[r : r + N, :], Yh[...], Yl[...])
            for row in range(0, N, 8):
                for u in range(2):
                    at = (r + row) * 2 + u * 8
                    W[e, at : at + 8, :] = part[row : row + 8, u * LANES : (u + 1) * LANES]

        def one(step, carry):
            tk, tg = peer(step)
            pltpu.make_async_remote_copy(
                src_ref=W.at[e, rows_of(tg, 16)],
                dst_ref=Q.at[e, rows_of(me, 16)],
                send_sem=back_sem,
                recv_sem=got_sem.at[e],
                device_id={"kpt": tk, "grid": tg},
                device_id_type=MESH,
            ).start()
            return carry

        lax.fori_loop(1, DEVICES, one, 0)
        Q[e, rows_of(me, 16), :] = W[e, rows_of(g, 16), :]

    solve(0)
    solve(1)

    def half_done(e, plane):
        parts = [Q[e, pl.ds(u * 8 + plane, LANES, stride=16), :] for u in range(2)]
        high, low = split(jnp.concatenate(parts, axis=1))
        cols = slice(e * LANES, (e + 1) * LANES)
        return dot3(tab[0, :, cols], tab[1, :, cols], high, low)

    def arrived(e):
        taken = Q.at[e, pl.ds(0, (DEVICES - 1) * 16)]
        pltpu.make_async_copy(taken, taken, got_sem.at[e]).wait()

    arrived(0)
    for plane in range(PLANES):
        half[plane] = half_done(0, plane)
    arrived(1)
    for plane in range(PLANES):
        high, low = split(half[plane] + half_done(1, plane))
        out[plane] = dot3(high, low, tab[2], tab[3])

    sent = R.at[:, pl.ds(0, (DEVICES - 1) * 16)]
    pltpu.make_async_copy(sent, sent, send_sem).wait()
    sent = Q.at[:, pl.ds(0, (DEVICES - 1) * 16)]
    pltpu.make_async_copy(sent, sent, back_sem).wait()


def on_device(orbitals, kweights, occupations, z_basis, z_eigen):
    any_space = pl.BlockSpec(memory_space=pl.ANY)
    smem = pl.BlockSpec(memory_space=pltpu.SMEM)
    vmem = pltpu.VMEM
    dma = pltpu.SemaphoreType.DMA
    return pl.pallas_call(
        kernel,
        out_shape=jax.ShapeDtypeStruct((PLANES, N, N), f32),
        in_specs=[any_space, smem, smem, any_space, any_space, any_space, any_space],
        out_specs=pl.BlockSpec(memory_space=vmem),
        scratch_shapes=[
            vmem((PLANES, 2, 2, 2, N, N), bf16),
            vmem((NZ, NZ), f32),
            vmem((1, NZ), f32),
            vmem((4, N, N), bf16),
            vmem((8, N), f32),
            vmem((2, 2, 1024, LANES), f32),
            vmem((2, 2048, LANES), f32),
            vmem((2, 1024, LANES), f32),
            vmem((2, 2048, LANES), f32),
            vmem((NZ, NZ), bf16),
            vmem((NZ, NZ), bf16),
            vmem((NZ, NZ), bf16),
            vmem((NZ, NZ), bf16),
            vmem((2, NZ, N), f32),
            vmem((2, N, N), bf16),
            vmem((2, N, N), bf16),
            vmem((NZ, N), bf16),
            vmem((NZ, N), bf16),
            vmem((NZ, N), bf16),
            vmem((NZ, N), bf16),
            vmem((PLANES, N, N), f32),
            dma((PLANES,)),
            dma((4,)),
            dma,
            dma((2,)),
            dma,
            dma((2,)),
            pltpu.SemaphoreType.REGULAR,
            pltpu.SemaphoreType.REGULAR,
            pltpu.SemaphoreType.REGULAR,
        ],
        compiler_params=pltpu.CompilerParams(
            collective_id=0, has_side_effects=True, vmem_limit_bytes=48 << 20
        ),
    )(
        orbitals, kweights, occupations, z_basis, z_eigen.reshape(1, NZ),
        jnp.asarray(tables()), jnp.asarray(mode_rows()),
    )


def solution(mesh):
    return jax.shard_map(
        on_device,
        mesh=mesh,
        in_specs=(P("kpt", None, None, "grid", None, None), P("kpt"), P("kpt", None), P(), P()),
        out_specs=P("grid", None, None),
        check_vma=False,
    )
```

```python
import functools

import jax
import jax.numpy as jnp
import numpy as np
from jax import lax
from jax.experimental import pallas as pl
from jax.experimental.pallas import tpu as pltpu
from jax.sharding import PartitionSpec as P

MESH = pl.DeviceIdType.MESH
f32 = jnp.float32
bf16 = jnp.bfloat16
N = 256
NZ = 512
LANES = 128
DEVICES = 128
PLANES = 8
QUAD = 4


def real_table():
    position = np.arange(N)
    angles = (position[:, None] * position[None, :] % N) * (2.0 * np.pi / N)
    return np.where(position[:, None] <= N // 2, np.cos(angles), np.sin(angles))


def tables():
    table = real_table()
    halves = []
    for one in (table.T, table):
        high = one.astype(bf16)
        low = (one - high.astype(np.float64)).astype(bf16)
        halves += [high, low]
    return np.stack(halves)


def mode_rows():
    position = np.arange(N)
    shift = (2.0 * np.sin(np.pi * position / N)) ** 2
    edges = (position == 0) | (position == N // 2)
    weight = np.where(edges, 1.0, 2.0) / N
    rows = np.zeros((8, N), np.float32)
    rows[0], rows[1] = shift, weight
    return rows


def split(value):
    high = value.astype(bf16)
    low = (value - high.astype(f32)).astype(bf16)
    return high, low


def dot(left, right):
    return jnp.dot(left, right, preferred_element_type=f32)


def dot3(left_high, left_low, right_high, right_low):
    return dot(left_high, right_high) + (dot(left_high, right_low) + dot(left_low, right_high))


def coords():
    k = lax.axis_index("kpt")
    g = lax.axis_index("grid")
    return g // 32 * 2 + k, lax.rem(g // 2, 4), lax.rem(g // 8, 4), lax.rem(g, 2)


def device(x, y, z, c):
    return lax.rem(x, 2), ((x // 2 * 4 + z) * 4 + y) * 2 + c


def for_each_peer(act):
    x, y, z, c = coords()
    across = []
    for step in (1, 3, 2, 0):
        tx = lax.rem(x + step, 4)
        for flip in range(2):
            across.append((lax.rem(tx, 2), tx // 2 * 32 + lax.rem(c + flip, 2)))

    def block(dy, dz, chosen):
        base = lax.rem(z + dz, 4) * 8 + lax.rem(y + dy, 4) * 2
        for tk, part in chosen:
            act(tk, base + part)

    def one(index, carry):
        block(lax.rem(index, 4), index // 4, across)
        return carry

    lax.fori_loop(1, 16, one, 0)
    block(0, 0, across[:6] + across[7:])


def rows_of(index, count):
    return pl.ds(pl.multiple_of(index * count, count), count)


def kernel(
    orb, kw_in, occ_in, zb, lam, tab_in, row_in, out,
    kwv, occv, obuf, zbuf, lamv, tab, rowv, B, R, W, Q, Zh, Zl, ZhT, ZlT, fac,
    dh, dl, Xh, Xl, Yh, Yl, half,
    orb_sem, in_sem, send_sem, recv_sem, back_sem, got_sem, column_sem,
):
    k = lax.axis_index("kpt")
    g = lax.axis_index("grid")
    me = k * 64 + g
    x, y, z, c = coords()

    def signal(sem, steps):
        for dx, dy, dz, dc in steps:
            tk, tg = device(
                lax.rem(x + dx, 4), lax.rem(y + dy, 4), lax.rem(z + dz, 4), lax.rem(c + dc, 2)
            )
            pl.semaphore_signal(sem, inc=1, device_id={"kpt": tk, "grid": tg}, device_id_type=MESH)

    plane_steps = [(i % 4, i // 4, 0, 0) for i in range(1, 16)]
    column_steps = [(0, 0, i % 4, i // 4) for i in range(1, 8)]
    barrier = pltpu.get_barrier_semaphore()
    signal(barrier, plane_steps + column_steps)

    def orb_copy(plane):
        return pltpu.make_async_copy(orb.at[:, :, :, plane], obuf.at[plane], orb_sem.at[plane])

    ins = [
        pltpu.make_async_copy(tab_in, tab, in_sem.at[0]),
        pltpu.make_async_copy(row_in, rowv, in_sem.at[1]),
        pltpu.make_async_copy(lam, lamv, in_sem.at[2]),
        pltpu.make_async_copy(zb, zbuf, in_sem.at[3]),
    ]
    scalars = [
        pltpu.make_async_copy(kw_in, kwv, in_sem.at[4]),
        pltpu.make_async_copy(occ_in, occv, in_sem.at[5]),
    ]
    for one in scalars:
        one.start()
    orb_copy(0).start()
    ins[0].start()
    for plane in range(1, PLANES):
        orb_copy(plane).start()
    for one in ins[1:]:
        one.start()

    for one in scalars:
        one.wait()
    weight = [[(kwv[p] * occv[p, b]).astype(f32) * (1.0 / 64.0) for b in range(2)] for p in range(2)]

    def plane_spectrum(plane):
        orb_copy(plane).wait()
        slot = plane % 2
        for r in range(0, N, 32):
            total = None
            for p in range(2):
                for b in range(2):
                    re = obuf[plane, p, b, 0, r : r + 32, :].astype(f32)
                    im = obuf[plane, p, b, 1, r : r + 32, :].astype(f32)
                    term = weight[p][b] * (re * re + im * im)
                    total = term if total is None else total + term
            high, low = split(total)
            dh[slot, r : r + 32, :] = high
            dl[slot, r : r + 32, :] = low
        along_y = dot3(dh[slot], dl[slot], tab[0], tab[1])
        high, low = split(along_y)
        both = dot3(tab[2], tab[3], high, low)
        h, q = plane // QUAD, plane % QUAD
        for e in range(2):
            for u in range(2):
                B[h, e, pl.ds(q * 2 + u, LANES, stride=8), :] = both[
                    e * LANES : (e + 1) * LANES, u * LANES : (u + 1) * LANES
                ]

    def send_out(h, e):
        def act(tk, tg):
            pltpu.make_async_remote_copy(
                src_ref=B.at[h, e, rows_of(tk * 64 + tg, 8)],
                dst_ref=R.at[e, rows_of(me * 2 + h, 8)],
                send_sem=send_sem,
                recv_sem=recv_sem.at[e],
                device_id={"kpt": tk, "grid": tg},
                device_id_type=MESH,
            ).start()

        for_each_peer(act)
        R[e, rows_of(me * 2 + h, 8), :] = B[h, e, rows_of(me, 8), :]

    ins[0].wait()
    plane_spectrum(0)
    plane_spectrum(1)
    pl.semaphore_wait(barrier, 22)
    signal(column_sem, column_steps)
    plane_spectrum(2)
    plane_spectrum(3)
    pl.semaphore_wait(column_sem, 7)
    send_out(0, 0)
    for plane in range(QUAD, PLANES):
        plane_spectrum(plane)
    send_out(1, 0)
    send_out(0, 1)
    send_out(1, 1)

    for one in ins[1:]:
        one.wait()
    for r in range(0, NZ, LANES):
        rows = zbuf[r : r + LANES, :]
        high, low = split(rows)
        Zh[r : r + LANES, :] = high
        Zl[r : r + LANES, :] = low
        turned = rows.T
        high, low = split(turned)
        ZhT[:, r : r + LANES] = high
        ZlT[:, r : r + LANES] = low
    shift_y, weight_y = rowv[0:1, :], rowv[1:2, :]
    lanes = lax.broadcasted_iota(jnp.int32, (1, N), 1)
    for e in range(2):
        mine = lanes == e * LANES + me
        shift_x = jnp.sum(jnp.where(mine, shift_y, 0.0), axis=1, keepdims=True)
        weight_x = jnp.sum(jnp.where(mine, weight_y, 0.0), axis=1, keepdims=True)
        for r in range(0, NZ, LANES):
            column = jnp.broadcast_to(lamv[0:1, r : r + LANES], (LANES, LANES)).T
            for u in range(2):
                cols = slice(u * LANES, (u + 1) * LANES)
                fac[e, r : r + LANES, cols] = (weight_y[:, cols] * weight_x) / (
                    column + (shift_y[:, cols] + shift_x)
                )

    upper = lax.broadcasted_iota(jnp.int32, (8, LANES), 0) < QUAD

    def solve(e):
        taken = R.at[e, pl.ds(0, (DEVICES - 1) * 16)]
        pltpu.make_async_copy(taken, taken, recv_sem.at[e]).wait()
        for u in range(2):
            cols = slice(u * LANES, (u + 1) * LANES)
            for r in range(0, NZ, LANES):
                first = R[e, pl.ds(r * 2 + u, LANES, stride=2), :]
                second = R[e, pl.ds(1024 + r * 2 + u, LANES, stride=2), :]
                high, low = split(first + second)
                Xh[r : r + LANES, cols] = high
                Xl[r : r + LANES, cols] = low
        for r in range(0, NZ, N):
            part = dot3(ZhT[r : r + N, :], ZlT[r : r + N, :], Xh[...], Xl[...])
            high, low = split(part * fac[e, r : r + N, :])
            Yh[r : r + N, :] = high
            Yl[r : r + N, :] = low
        for r in range(0, NZ, N):
            part = dot3(Zh[r : r + N, :], Zl[r : r + N, :], Yh[...], Yl[...])
            for row in range(0, N, 8):
                first = part[row : row + 8, :LANES]
                second = part[row : row + 8, LANES:]
                at = slice(r + row, r + row + 8)
                W[e, 0, at, :] = jnp.where(upper, first, pltpu.roll(second, QUAD, 0))
                W[e, 1, at, :] = jnp.where(upper, pltpu.roll(first, QUAD, 0), second)

    def send_back(e, h):
        def act(tk, tg):
            pltpu.make_async_remote_copy(
                src_ref=W.at[e, h, rows_of(tg, 8)],
                dst_ref=Q.at[e, h, rows_of(me, 8)],
                send_sem=back_sem,
                recv_sem=got_sem.at[e + h * e],
                device_id={"kpt": tk, "grid": tg},
                device_id_type=MESH,
            ).start()

        for_each_peer(act)
        Q[e, h, rows_of(me, 8), :] = W[e, h, rows_of(g, 8), :]

    solve(0)
    send_back(0, 0)
    send_back(0, 1)
    solve(1)
    send_back(1, 0)
    send_back(1, 1)

    def half_done(e, plane):
        h, q = plane // QUAD, plane % QUAD
        parts = [Q[e, h, pl.ds(u * QUAD + q, LANES, stride=8), :] for u in range(2)]
        high, low = split(jnp.concatenate(parts, axis=1))
        cols = slice(e * LANES, (e + 1) * LANES)
        return dot3(tab[0, :, cols], tab[1, :, cols], high, low)

    def arrived(taken, sem):
        pltpu.make_async_copy(taken, taken, sem).wait()

    arrived(Q.at[0, :, pl.ds(0, (DEVICES - 1) * 8)], got_sem.at[0])
    for plane in range(PLANES):
        half[plane] = half_done(0, plane)
    for h in range(2):
        arrived(Q.at[1, h, pl.ds(0, (DEVICES - 1) * 8)], got_sem.at[1 + h])
        for plane in range(h * QUAD, (h + 1) * QUAD):
            high, low = split(half[plane] + half_done(1, plane))
            out[plane] = dot3(high, low, tab[2], tab[3])

    arrived(R.at[:, pl.ds(0, (DEVICES - 1) * 16)], send_sem)
    arrived(Q.at[:, :, pl.ds(0, (DEVICES - 1) * 8)], back_sem)


def on_device(orbitals, kweights, occupations, z_basis, z_eigen):
    hbm = pl.BlockSpec(memory_space=pltpu.HBM)
    vmem = pltpu.VMEM
    dma = pltpu.SemaphoreType.DMA
    return pl.pallas_call(
        kernel,
        out_shape=jax.ShapeDtypeStruct((PLANES, N, N), f32),
        in_specs=[hbm] * 7,
        out_specs=pl.BlockSpec(memory_space=vmem),
        scratch_shapes=[
            pltpu.SMEM((2,), jnp.int32),
            pltpu.SMEM((2, 2), jnp.int32),
            vmem((PLANES, 2, 2, 2, N, N), bf16),
            vmem((NZ, NZ), f32),
            vmem((1, NZ), f32),
            vmem((4, N, N), bf16),
            vmem((8, N), f32),
            vmem((2, 2, 1024, LANES), f32),
            vmem((2, 2048, LANES), f32),
            vmem((2, 2, 512, LANES), f32),
            vmem((2, 2, 1024, LANES), f32),
            vmem((NZ, NZ), bf16),
            vmem((NZ, NZ), bf16),
            vmem((NZ, NZ), bf16),
            vmem((NZ, NZ), bf16),
            vmem((2, NZ, N), f32),
            vmem((2, N, N), bf16),
            vmem((2, N, N), bf16),
            vmem((NZ, N), bf16),
            vmem((NZ, N), bf16),
            vmem((NZ, N), bf16),
            vmem((NZ, N), bf16),
            vmem((PLANES, N, N), f32),
            dma((PLANES,)),
            dma((6,)),
            dma,
            dma((2,)),
            dma,
            dma((3,)),
            pltpu.SemaphoreType.REGULAR,
        ],
        compiler_params=pltpu.CompilerParams(
            collective_id=0, has_side_effects=True, vmem_limit_bytes=48 << 20
        ),
    )(*(pltpu.with_memory_space_constraint(one, pltpu.HBM) for one in (
        orbitals, kweights, occupations, z_basis, z_eigen.reshape(1, NZ),
        jnp.asarray(tables()), jnp.asarray(mode_rows()),
    )))


def solution(mesh):
    return jax.shard_map(
        on_device,
        mesh=mesh,
        in_specs=(P("kpt", None, None, "grid", None, None), P("kpt"), P("kpt", None), P(), P()),
        out_specs=P("grid", None, None),
        check_vma=False,
    )
```

```python
import functools

import jax
import jax.numpy as jnp
import numpy as np
from jax import lax
from jax.experimental import pallas as pl
from jax.experimental.pallas import tpu as pltpu
from jax.sharding import PartitionSpec as P

MESH = pl.DeviceIdType.MESH
f32 = jnp.float32
bf16 = jnp.bfloat16
N = 256
NZ = 512
LANES = 128
DEVICES = 128
PLANES = 8
QUAD = 4


def real_table():
    position = np.arange(N)
    angles = (position[:, None] * position[None, :] % N) * (2.0 * np.pi / N)
    return np.where(position[:, None] <= N // 2, np.cos(angles), np.sin(angles))


def tables():
    table = real_table()
    halves = []
    for one in (table.T, table):
        high = one.astype(bf16)
        low = (one - high.astype(np.float64)).astype(bf16)
        halves += [high, low]
    return np.stack(halves)


def mode_rows():
    position = np.arange(N)
    shift = (2.0 * np.sin(np.pi * position / N)) ** 2
    edges = (position == 0) | (position == N // 2)
    weight = np.where(edges, 1.0, 2.0) / N
    rows = np.zeros((8, N), np.float32)
    rows[0], rows[1] = shift, weight
    return rows


def split(value):
    high = value.astype(bf16)
    low = (value - high.astype(f32)).astype(bf16)
    return high, low


def dot(left, right):
    return jnp.dot(left, right, preferred_element_type=f32)


def dot3(left_high, left_low, right_high, right_low):
    return dot(left_high, right_high) + (dot(left_high, right_low) + dot(left_low, right_high))


def coords():
    k = lax.axis_index("kpt")
    g = lax.axis_index("grid")
    return g // 32 * 2 + k, lax.rem(g // 2, 4), lax.rem(g // 8, 4), lax.rem(g, 2)


def device(x, y, z, c):
    return lax.rem(x, 2), ((x // 2 * 4 + z) * 4 + y) * 2 + c


def for_each_peer(act):
    x, y, z, c = coords()
    across = []
    for step in (1, 3, 2, 0):
        tx = lax.rem(x + step, 4)
        for flip in range(2):
            across.append((lax.rem(tx, 2), tx // 2 * 32 + lax.rem(c + flip, 2)))

    def block(dy, dz, chosen):
        base = lax.rem(z + dz, 4) * 8 + lax.rem(y + dy, 4) * 2
        for tk, part in chosen:
            act(tk, base + part)

    def one(index, carry):
        block(lax.rem(index, 4), index // 4, across)
        return carry

    lax.fori_loop(1, 16, one, 0)
    block(0, 0, across[:6] + across[7:])


def rows_of(index, count):
    return pl.ds(pl.multiple_of(index * count, count), count)


def kernel(
    orb, kw_in, occ_in, zb, lam, tab_in, row_in, out,
    kwv, occv, obuf, zbuf, lamv, to_ky, to_jx, from_jx, from_ky, rowv, B, R, W, Q, Zh, Zl, ZhT, ZlT, fac,
    dcat, ecat, Xh, Xl, Yh, Yl, half, fcat, acat,
    orb_sem, in_sem, tab_sem, send_sem, recv_sem, back_sem, got_sem, column_sem,
):
    k = lax.axis_index("kpt")
    g = lax.axis_index("grid")
    me = k * 64 + g
    x, y, z, c = coords()

    def signal(sem, steps):
        for dx, dy, dz, dc in steps:
            tk, tg = device(
                lax.rem(x + dx, 4), lax.rem(y + dy, 4), lax.rem(z + dz, 4), lax.rem(c + dc, 2)
            )
            pl.semaphore_signal(sem, inc=1, device_id={"kpt": tk, "grid": tg}, device_id_type=MESH)

    plane_steps = [(i % 4, i // 4, 0, 0) for i in range(1, 16)]
    column_steps = [(0, 0, i % 4, i // 4) for i in range(1, 8)]
    barrier = pltpu.get_barrier_semaphore()
    signal(barrier, plane_steps + column_steps)

    def orb_copy(plane):
        return pltpu.make_async_copy(orb.at[:, :, :, plane], obuf.at[plane], orb_sem.at[plane])

    ins = [
        pltpu.make_async_copy(row_in, rowv, in_sem.at[1]),
        pltpu.make_async_copy(lam, lamv, in_sem.at[2]),
        pltpu.make_async_copy(zb, zbuf, in_sem.at[3]),
    ]
    scalars = [
        pltpu.make_async_copy(kw_in, kwv, in_sem.at[4]),
        pltpu.make_async_copy(occ_in, occv, in_sem.at[5]),
    ]
    for one in scalars:
        one.start()

    def table_copies(lo, hi):
        sources = [tab_in.at[0], tab_in.at[1], tab_in.at[0], tab_in.at[2], tab_in.at[2], tab_in.at[3]]
        sources += [
            tab_in.at[part, :, e * LANES : (e + 1) * LANES] for e in range(2) for part in (0, 0, 1)
        ]
        sources += [tab_in.at[2], tab_in.at[3], tab_in.at[2]]
        targets = [to_ky.at[i * N : (i + 1) * N] for i in range(3)]
        targets += [to_jx.at[:, i * N : (i + 1) * N] for i in range(3)]
        targets += [
            from_jx.at[e, :, i * LANES : (i + 1) * LANES] for e in range(2) for i in range(3)
        ]
        targets += [from_ky.at[i * N : (i + 1) * N] for i in range(3)]
        return [
            pltpu.make_async_copy(sources[i], targets[i], tab_sem.at[i]) for i in range(lo, hi)
        ]

    orb_copy(0).start()
    for one in table_copies(0, 6):
        one.start()
    for plane in range(1, PLANES):
        orb_copy(plane).start()
    for one in table_copies(6, 15) + ins:
        one.start()

    for one in scalars:
        one.wait()
    weight = [[(kwv[p] * occv[p, b]).astype(f32) * (1.0 / 64.0) for b in range(2)] for p in range(2)]

    def plane_spectrum(plane):
        orb_copy(plane).wait()
        slot = plane % 2
        for r in range(0, N, 32):
            total = None
            for p in range(2):
                for b in range(2):
                    re = obuf[plane, p, b, 0, r : r + 32, :].astype(f32)
                    im = obuf[plane, p, b, 1, r : r + 32, :].astype(f32)
                    term = weight[p][b] * (re * re + im * im)
                    total = term if total is None else total + term
            high, low = split(total)
            dcat[slot, r : r + 32, 0:N] = high
            dcat[slot, r : r + 32, N : 2 * N] = high
            dcat[slot, r : r + 32, 2 * N : 3 * N] = low
        if plane == 0:
            for one in table_copies(0, 6):
                one.wait()
        high, low = split(dot(dcat[slot], to_ky[...]))
        ecat[slot, 0:N, :] = high
        ecat[slot, N : 2 * N, :] = low
        ecat[slot, 2 * N : 3 * N, :] = high
        both = dot(to_jx[...], ecat[slot])
        h, q = plane // QUAD, plane % QUAD
        for e in range(2):
            for u in range(2):
                B[h, e, pl.ds(q * 2 + u, LANES, stride=8), :] = both[
                    e * LANES : (e + 1) * LANES, u * LANES : (u + 1) * LANES
                ]

    def send_out(h, e):
        def act(tk, tg):
            pltpu.make_async_remote_copy(
                src_ref=B.at[h, e, rows_of(tk * 64 + tg, 8)],
                dst_ref=R.at[e, rows_of(me * 2 + h, 8)],
                send_sem=send_sem,
                recv_sem=recv_sem.at[e],
                device_id={"kpt": tk, "grid": tg},
                device_id_type=MESH,
            ).start()

        for_each_peer(act)
        R[e, rows_of(me * 2 + h, 8), :] = B[h, e, rows_of(me, 8), :]

    plane_spectrum(0)
    pl.semaphore_wait(barrier, 22)
    signal(column_sem, column_steps)
    plane_spectrum(1)
    plane_spectrum(2)
    plane_spectrum(3)
    pl.semaphore_wait(column_sem, 7)
    send_out(0, 0)
    for plane in range(QUAD, PLANES):
        plane_spectrum(plane)
    send_out(1, 0)
    send_out(0, 1)
    send_out(1, 1)

    for one in table_copies(6, 15) + ins:
        one.wait()
    for r in range(0, NZ, LANES):
        rows = zbuf[r : r + LANES, :]
        high, low = split(rows)
        Zh[r : r + LANES, :] = high
        Zl[r : r + LANES, :] = low
        turned = rows.T
        high, low = split(turned)
        ZhT[:, r : r + LANES] = high
        ZlT[:, r : r + LANES] = low
    shift_y, weight_y = rowv[0:1, :], rowv[1:2, :]
    lanes = lax.broadcasted_iota(jnp.int32, (1, N), 1)
    for e in range(2):
        mine = lanes == e * LANES + me
        shift_x = jnp.sum(jnp.where(mine, shift_y, 0.0), axis=1, keepdims=True)
        weight_x = jnp.sum(jnp.where(mine, weight_y, 0.0), axis=1, keepdims=True)
        for r in range(0, NZ, LANES):
            column = jnp.broadcast_to(lamv[0:1, r : r + LANES], (LANES, LANES)).T
            for u in range(2):
                cols = slice(u * LANES, (u + 1) * LANES)
                fac[e, r : r + LANES, cols] = (weight_y[:, cols] * weight_x) / (
                    column + (shift_y[:, cols] + shift_x)
                )

    upper = lax.broadcasted_iota(jnp.int32, (8, LANES), 0) < QUAD

    def solve(e):
        taken = R.at[e, pl.ds(0, (DEVICES - 1) * 16)]
        pltpu.make_async_copy(taken, taken, recv_sem.at[e]).wait()
        for u in range(2):
            cols = slice(u * LANES, (u + 1) * LANES)
            for r in range(0, NZ, LANES):
                first = R[e, pl.ds(r * 2 + u, LANES, stride=2), :]
                second = R[e, pl.ds(1024 + r * 2 + u, LANES, stride=2), :]
                high, low = split(first + second)
                Xh[r : r + LANES, cols] = high
                Xl[r : r + LANES, cols] = low
        for r in range(0, NZ, N):
            part = dot3(ZhT[r : r + N, :], ZlT[r : r + N, :], Xh[...], Xl[...])
            high, low = split(part * fac[e, r : r + N, :])
            Yh[r : r + N, :] = high
            Yl[r : r + N, :] = low
        for r in range(0, NZ, N):
            part = dot3(Zh[r : r + N, :], Zl[r : r + N, :], Yh[...], Yl[...])
            for row in range(0, N, 8):
                first = part[row : row + 8, :LANES]
                second = part[row : row + 8, LANES:]
                at = slice(r + row, r + row + 8)
                W[e, 0, at, :] = jnp.where(upper, first, pltpu.roll(second, QUAD, 0))
                W[e, 1, at, :] = jnp.where(upper, pltpu.roll(first, QUAD, 0), second)

    def send_back(e, h):
        def act(tk, tg):
            pltpu.make_async_remote_copy(
                src_ref=W.at[e, h, rows_of(tg, 8)],
                dst_ref=Q.at[e, h, rows_of(me, 8)],
                send_sem=back_sem,
                recv_sem=got_sem.at[e + h * e],
                device_id={"kpt": tk, "grid": tg},
                device_id_type=MESH,
            ).start()

        for_each_peer(act)
        Q[e, h, rows_of(me, 8), :] = W[e, h, rows_of(g, 8), :]

    solve(0)
    send_back(0, 0)
    send_back(0, 1)
    solve(1)
    send_back(1, 0)
    send_back(1, 1)

    def half_done(e, plane):
        h, q = plane // QUAD, plane % QUAD
        parts = [Q[e, h, pl.ds(u * QUAD + q, LANES, stride=8), :] for u in range(2)]
        high, low = split(jnp.concatenate(parts, axis=1))
        slot = plane % 2
        fcat[slot, 0:LANES, :] = high
        fcat[slot, LANES : 2 * LANES, :] = low
        fcat[slot, 2 * LANES : 3 * LANES, :] = high
        return dot(from_jx[e], fcat[slot])

    def arrived(taken, sem):
        pltpu.make_async_copy(taken, taken, sem).wait()

    arrived(Q.at[0, :, pl.ds(0, (DEVICES - 1) * 8)], got_sem.at[0])
    for plane in range(PLANES):
        half[plane] = half_done(0, plane)
    for h in range(2):
        arrived(Q.at[1, h, pl.ds(0, (DEVICES - 1) * 8)], got_sem.at[1 + h])
        for plane in range(h * QUAD, (h + 1) * QUAD):
            high, low = split(half[plane] + half_done(1, plane))
            slot = plane % 2
            acat[slot, :, 0:N] = high
            acat[slot, :, N : 2 * N] = high
            acat[slot, :, 2 * N : 3 * N] = low
            out[plane] = dot(acat[slot], from_ky[...])

    arrived(R.at[:, pl.ds(0, (DEVICES - 1) * 16)], send_sem)
    arrived(Q.at[:, :, pl.ds(0, (DEVICES - 1) * 8)], back_sem)


def on_device(orbitals, kweights, occupations, z_basis, z_eigen):
    hbm = pl.BlockSpec(memory_space=pltpu.HBM)
    vmem = pltpu.VMEM
    dma = pltpu.SemaphoreType.DMA
    return pl.pallas_call(
        kernel,
        out_shape=jax.ShapeDtypeStruct((PLANES, N, N), f32),
        in_specs=[hbm] * 7,
        out_specs=pl.BlockSpec(memory_space=vmem),
        scratch_shapes=[
            pltpu.SMEM((2,), jnp.int32),
            pltpu.SMEM((2, 2), jnp.int32),
            vmem((PLANES, 2, 2, 2, N, N), bf16),
            vmem((NZ, NZ), f32),
            vmem((1, NZ), f32),
            vmem((3 * N, N), bf16),
            vmem((N, 3 * N), bf16),
            vmem((2, N, 3 * LANES), bf16),
            vmem((3 * N, N), bf16),
            vmem((8, N), f32),
            vmem((2, 2, 1024, LANES), f32),
            vmem((2, 2048, LANES), f32),
            vmem((2, 2, 512, LANES), f32),
            vmem((2, 2, 1024, LANES), f32),
            vmem((NZ, NZ), bf16),
            vmem((NZ, NZ), bf16),
            vmem((NZ, NZ), bf16),
            vmem((NZ, NZ), bf16),
            vmem((2, NZ, N), f32),
            vmem((2, N, 3 * N), bf16),
            vmem((2, 3 * N, N), bf16),
            vmem((NZ, N), bf16),
            vmem((NZ, N), bf16),
            vmem((NZ, N), bf16),
            vmem((NZ, N), bf16),
            vmem((PLANES, N, N), f32),
            vmem((2, 3 * LANES, N), bf16),
            vmem((2, N, 3 * N), bf16),
            dma((PLANES,)),
            dma((6,)),
            dma((15,)),
            dma,
            dma((2,)),
            dma,
            dma((3,)),
            pltpu.SemaphoreType.REGULAR,
        ],
        compiler_params=pltpu.CompilerParams(
            collective_id=0, has_side_effects=True, vmem_limit_bytes=48 << 20
        ),
    )(*(pltpu.with_memory_space_constraint(one, pltpu.HBM) for one in (
        orbitals, kweights, occupations, z_basis, z_eigen.reshape(1, NZ),
        jnp.asarray(tables()), jnp.asarray(mode_rows()),
    )))


def solution(mesh):
    return jax.shard_map(
        on_device,
        mesh=mesh,
        in_specs=(P("kpt", None, None, "grid", None, None), P("kpt"), P("kpt", None), P(), P()),
        out_specs=P("grid", None, None),
        check_vma=False,
    )
```

```python
import functools

import jax
import jax.numpy as jnp
import numpy as np
from jax import lax
from jax.experimental import pallas as pl
from jax.experimental.pallas import tpu as pltpu
from jax.sharding import PartitionSpec as P

MESH = pl.DeviceIdType.MESH
f32 = jnp.float32
bf16 = jnp.bfloat16
N = 256
NZ = 512
LANES = 128
DEVICES = 128
PLANES = 8
QUAD = 4


def real_table():
    position = np.arange(N)
    angles = (position[:, None] * position[None, :] % N) * (2.0 * np.pi / N)
    return np.where(position[:, None] <= N // 2, np.cos(angles), np.sin(angles))


def tables():
    table = real_table()
    halves = []
    for one in (table.T, table):
        high = one.astype(bf16)
        low = (one - high.astype(np.float64)).astype(bf16)
        halves += [high, low]
    return np.stack(halves)


def mode_rows():
    position = np.arange(N)
    shift = (2.0 * np.sin(np.pi * position / N)) ** 2
    edges = (position == 0) | (position == N // 2)
    weight = np.where(edges, 1.0, 2.0) / N
    rows = np.zeros((8, N), np.float32)
    rows[0], rows[1] = shift, weight
    return rows


def split(value):
    high = value.astype(bf16)
    low = (value - high.astype(f32)).astype(bf16)
    return high, low


def dot(left, right):
    return jnp.dot(left, right, preferred_element_type=f32)


def dot3(left_high, left_low, right_high, right_low):
    return dot(left_high, right_high) + (dot(left_high, right_low) + dot(left_low, right_high))


def coords():
    k = lax.axis_index("kpt")
    g = lax.axis_index("grid")
    return g // 32 * 2 + k, lax.rem(g // 2, 4), lax.rem(g // 8, 4), lax.rem(g, 2)


def device(x, y, z, c):
    return lax.rem(x, 2), ((x // 2 * 4 + z) * 4 + y) * 2 + c


def for_each_peer(act):
    x, y, z, c = coords()
    across = []
    for step in (1, 3, 2, 0):
        tx = lax.rem(x + step, 4)
        for flip in range(2):
            across.append((lax.rem(tx, 2), tx // 2 * 32 + lax.rem(c + flip, 2)))

    def block(dy, dz, chosen):
        base = lax.rem(z + dz, 4) * 8 + lax.rem(y + dy, 4) * 2
        for tk, part in chosen:
            act(tk, base + part)

    def one(index, carry):
        block(lax.rem(index, 4), index // 4, across)
        return carry

    lax.fori_loop(1, 16, one, 0)
    block(0, 0, across[:6] + across[7:])


def rows_of(index, count):
    return pl.ds(pl.multiple_of(index * count, count), count)


def kernel(
    orb, kw_in, occ_in, zb, lam, tab_in, row_in, out,
    kwv, occv, obuf, zbuf, lamv, to_ky, to_jx, from_jx, from_ky, rowv, B, R, W, Q, Zh, Zl, ZhT, ZlT, fac,
    density, Xh, Xl, Yh, Yl, half, fcat, acat,
    orb_sem, in_sem, tab_sem, send_sem, recv_sem, back_sem, got_sem, column_sem,
):
    k = lax.axis_index("kpt")
    g = lax.axis_index("grid")
    me = k * 64 + g
    x, y, z, c = coords()

    def signal(sem, steps):
        for dx, dy, dz, dc in steps:
            tk, tg = device(
                lax.rem(x + dx, 4), lax.rem(y + dy, 4), lax.rem(z + dz, 4), lax.rem(c + dc, 2)
            )
            pl.semaphore_signal(sem, inc=1, device_id={"kpt": tk, "grid": tg}, device_id_type=MESH)

    plane_steps = [(i % 4, i // 4, 0, 0) for i in range(1, 16)]
    column_steps = [(0, 0, i % 4, i // 4) for i in range(1, 8)]
    barrier = pltpu.get_barrier_semaphore()
    signal(barrier, plane_steps + column_steps)

    def orb_copy(plane):
        return pltpu.make_async_copy(orb.at[:, :, :, plane], obuf.at[plane], orb_sem.at[plane])

    ins = [
        pltpu.make_async_copy(row_in, rowv, in_sem.at[1]),
        pltpu.make_async_copy(lam, lamv, in_sem.at[2]),
        pltpu.make_async_copy(zb, zbuf, in_sem.at[3]),
    ]
    scalars = [
        pltpu.make_async_copy(kw_in, kwv, in_sem.at[4]),
        pltpu.make_async_copy(occ_in, occv, in_sem.at[5]),
    ]
    for one in scalars:
        one.start()

    def table_copies(lo, hi):
        sources = [tab_in.at[0], tab_in.at[1], tab_in.at[2], tab_in.at[3]]
        sources += [
            tab_in.at[part, :, e * LANES : (e + 1) * LANES] for e in range(2) for part in (0, 0, 1)
        ]
        sources += [tab_in.at[2], tab_in.at[3], tab_in.at[2]]
        targets = [to_ky.at[0], to_ky.at[1], to_jx.at[0], to_jx.at[1]]
        targets += [
            from_jx.at[e, :, i * LANES : (i + 1) * LANES] for e in range(2) for i in range(3)
        ]
        targets += [from_ky.at[i * N : (i + 1) * N] for i in range(3)]
        return [
            pltpu.make_async_copy(sources[i], targets[i], tab_sem.at[i]) for i in range(lo, hi)
        ]

    orb_copy(0).start()
    for one in table_copies(0, 4):
        one.start()
    for plane in range(1, PLANES):
        orb_copy(plane).start()
    for one in table_copies(4, 13) + ins:
        one.start()

    for one in scalars:
        one.wait()
    weight = [[(kwv[p] * occv[p, b]).astype(f32) * (1.0 / 64.0) for b in range(2)] for p in range(2)]

    def plane_spectrum(plane):
        orb_copy(plane).wait()
        slot = plane % 2
        for r in range(0, N, 32):
            total = None
            for p in range(2):
                for b in range(2):
                    re = obuf[plane, p, b, 0, r : r + 32, :].astype(f32)
                    im = obuf[plane, p, b, 1, r : r + 32, :].astype(f32)
                    term = weight[p][b] * (re * re + im * im)
                    total = term if total is None else total + term
            high, low = split(total)
            density[slot, 0, r : r + 32, :] = high
            density[slot, 1, r : r + 32, :] = low
        if plane == 0:
            for one in table_copies(0, 4):
                one.wait()
        high, low = split(dot3(density[slot, 0], density[slot, 1], to_ky[0], to_ky[1]))
        both = dot3(to_jx[0], to_jx[1], high, low)
        h, q = plane // QUAD, plane % QUAD
        for e in range(2):
            for u in range(2):
                B[h, e, pl.ds(q * 2 + u, LANES, stride=8), :] = both[
                    e * LANES : (e + 1) * LANES, u * LANES : (u + 1) * LANES
                ]

    def send_out(h, e):
        def act(tk, tg):
            pltpu.make_async_remote_copy(
                src_ref=B.at[h, e, rows_of(tk * 64 + tg, 8)],
                dst_ref=R.at[e, rows_of(me * 2 + h, 8)],
                send_sem=send_sem,
                recv_sem=recv_sem.at[e],
                device_id={"kpt": tk, "grid": tg},
                device_id_type=MESH,
            ).start()

        for_each_peer(act)
        R[e, rows_of(me * 2 + h, 8), :] = B[h, e, rows_of(me, 8), :]

    plane_spectrum(0)
    pl.semaphore_wait(barrier, 22)
    signal(column_sem, column_steps)
    plane_spectrum(1)
    plane_spectrum(2)
    plane_spectrum(3)
    pl.semaphore_wait(column_sem, 7)
    send_out(0, 0)
    for plane in range(QUAD, PLANES):
        plane_spectrum(plane)
    send_out(1, 0)
    send_out(0, 1)
    send_out(1, 1)

    for one in table_copies(4, 13) + ins:
        one.wait()
    for r in range(0, NZ, LANES):
        rows = zbuf[r : r + LANES, :]
        high, low = split(rows)
        Zh[r : r + LANES, :] = high
        Zl[r : r + LANES, :] = low
        turned = rows.T
        high, low = split(turned)
        ZhT[:, r : r + LANES] = high
        ZlT[:, r : r + LANES] = low
    shift_y, weight_y = rowv[0:1, :], rowv[1:2, :]
    lanes = lax.broadcasted_iota(jnp.int32, (1, N), 1)
    for e in range(2):
        mine = lanes == e * LANES + me
        shift_x = jnp.sum(jnp.where(mine, shift_y, 0.0), axis=1, keepdims=True)
        weight_x = jnp.sum(jnp.where(mine, weight_y, 0.0), axis=1, keepdims=True)
        for r in range(0, NZ, LANES):
            column = jnp.broadcast_to(lamv[0:1, r : r + LANES], (LANES, LANES)).T
            for u in range(2):
                cols = slice(u * LANES, (u + 1) * LANES)
                fac[e, r : r + LANES, cols] = (weight_y[:, cols] * weight_x) / (
                    column + (shift_y[:, cols] + shift_x)
                )

    upper = lax.broadcasted_iota(jnp.int32, (8, LANES), 0) < QUAD

    def solve(e):
        taken = R.at[e, pl.ds(0, (DEVICES - 1) * 16)]
        pltpu.make_async_copy(taken, taken, recv_sem.at[e]).wait()
        for u in range(2):
            cols = slice(u * LANES, (u + 1) * LANES)
            for r in range(0, NZ, LANES):
                first = R[e, pl.ds(r * 2 + u, LANES, stride=2), :]
                second = R[e, pl.ds(1024 + r * 2 + u, LANES, stride=2), :]
                high, low = split(first + second)
                Xh[r : r + LANES, cols] = high
                Xl[r : r + LANES, cols] = low
        for r in range(0, NZ, N):
            part = dot3(ZhT[r : r + N, :], ZlT[r : r + N, :], Xh[...], Xl[...])
            high, low = split(part * fac[e, r : r + N, :])
            Yh[r : r + N, :] = high
            Yl[r : r + N, :] = low
        for r in range(0, NZ, N):
            part = dot3(Zh[r : r + N, :], Zl[r : r + N, :], Yh[...], Yl[...])
            for row in range(0, N, 8):
                first = part[row : row + 8, :LANES]
                second = part[row : row + 8, LANES:]
                at = slice(r + row, r + row + 8)
                W[e, 0, at, :] = jnp.where(upper, first, pltpu.roll(second, QUAD, 0))
                W[e, 1, at, :] = jnp.where(upper, pltpu.roll(first, QUAD, 0), second)

    def send_back(e, h):
        def act(tk, tg):
            pltpu.make_async_remote_copy(
                src_ref=W.at[e, h, rows_of(tg, 8)],
                dst_ref=Q.at[e, h, rows_of(me, 8)],
                send_sem=back_sem,
                recv_sem=got_sem.at[e + h * e],
                device_id={"kpt": tk, "grid": tg},
                device_id_type=MESH,
            ).start()

        for_each_peer(act)
        Q[e, h, rows_of(me, 8), :] = W[e, h, rows_of(g, 8), :]

    solve(0)
    send_back(0, 0)
    send_back(0, 1)
    solve(1)
    send_back(1, 0)
    send_back(1, 1)

    def half_done(e, plane):
        h, q = plane // QUAD, plane % QUAD
        parts = [Q[e, h, pl.ds(u * QUAD + q, LANES, stride=8), :] for u in range(2)]
        high, low = split(jnp.concatenate(parts, axis=1))
        slot = plane % 2
        fcat[slot, 0:LANES, :] = high
        fcat[slot, LANES : 2 * LANES, :] = low
        fcat[slot, 2 * LANES : 3 * LANES, :] = high
        return dot(from_jx[e], fcat[slot])

    def arrived(taken, sem):
        pltpu.make_async_copy(taken, taken, sem).wait()

    arrived(Q.at[0, :, pl.ds(0, (DEVICES - 1) * 8)], got_sem.at[0])
    for plane in range(PLANES):
        half[plane] = half_done(0, plane)
    for h in range(2):
        arrived(Q.at[1, h, pl.ds(0, (DEVICES - 1) * 8)], got_sem.at[1 + h])
        for plane in range(h * QUAD, (h + 1) * QUAD):
            high, low = split(half[plane] + half_done(1, plane))
            at = slice(plane % QUAD * N, (plane % QUAD + 1) * N)
            acat[at, 0:N] = high
            acat[at, N : 2 * N] = high
            acat[at, 2 * N : 3 * N] = low
        out[h * QUAD : (h + 1) * QUAD] = dot(acat[...], from_ky[...]).reshape(QUAD, N, N)

    arrived(R.at[:, pl.ds(0, (DEVICES - 1) * 16)], send_sem)
    arrived(Q.at[:, :, pl.ds(0, (DEVICES - 1) * 8)], back_sem)


def on_device(orbitals, kweights, occupations, z_basis, z_eigen):
    hbm = pl.BlockSpec(memory_space=pltpu.HBM)
    vmem = pltpu.VMEM
    dma = pltpu.SemaphoreType.DMA
    return pl.pallas_call(
        kernel,
        out_shape=jax.ShapeDtypeStruct((PLANES, N, N), f32),
        in_specs=[hbm] * 7,
        out_specs=pl.BlockSpec(memory_space=vmem),
        scratch_shapes=[
            pltpu.SMEM((2,), jnp.int32),
            pltpu.SMEM((2, 2), jnp.int32),
            vmem((PLANES, 2, 2, 2, N, N), bf16),
            vmem((NZ, NZ), f32),
            vmem((1, NZ), f32),
            vmem((2, N, N), bf16),
            vmem((2, N, N), bf16),
            vmem((2, N, 3 * LANES), bf16),
            vmem((3 * N, N), bf16),
            vmem((8, N), f32),
            vmem((2, 2, 1024, LANES), f32),
            vmem((2, 2048, LANES), f32),
            vmem((2, 2, 512, LANES), f32),
            vmem((2, 2, 1024, LANES), f32),
            vmem((NZ, NZ), bf16),
            vmem((NZ, NZ), bf16),
            vmem((NZ, NZ), bf16),
            vmem((NZ, NZ), bf16),
            vmem((2, NZ, N), f32),
            vmem((2, 2, N, N), bf16),
            vmem((NZ, N), bf16),
            vmem((NZ, N), bf16),
            vmem((NZ, N), bf16),
            vmem((NZ, N), bf16),
            vmem((PLANES, N, N), f32),
            vmem((2, 3 * LANES, N), bf16),
            vmem((QUAD * N, 3 * N), bf16),
            dma((PLANES,)),
            dma((6,)),
            dma((13,)),
            dma,
            dma((2,)),
            dma,
            dma((3,)),
            pltpu.SemaphoreType.REGULAR,
        ],
        compiler_params=pltpu.CompilerParams(
            collective_id=0, has_side_effects=True, vmem_limit_bytes=48 << 20
        ),
    )(*(pltpu.with_memory_space_constraint(one, pltpu.HBM) for one in (
        orbitals, kweights, occupations, z_basis, z_eigen.reshape(1, NZ),
        jnp.asarray(tables()), jnp.asarray(mode_rows()),
    )))


def solution(mesh):
    return jax.shard_map(
        on_device,
        mesh=mesh,
        in_specs=(P("kpt", None, None, "grid", None, None), P("kpt"), P("kpt", None), P(), P()),
        out_specs=P("grid", None, None),
        check_vma=False,
    )
```

```python
import functools

import jax
import jax.numpy as jnp
import numpy as np
from jax import lax
from jax.experimental import pallas as pl
from jax.experimental.pallas import tpu as pltpu
from jax.sharding import PartitionSpec as P

MESH = pl.DeviceIdType.MESH
f32 = jnp.float32
bf16 = jnp.bfloat16
N = 256
NZ = 512
LANES = 128
DEVICES = 128
PLANES = 8
QUAD = 4


def real_table():
    position = np.arange(N)
    angles = (position[:, None] * position[None, :] % N) * (2.0 * np.pi / N)
    return np.where(position[:, None] <= N // 2, np.cos(angles), np.sin(angles))


def tables():
    table = real_table()
    halves = []
    for one in (table.T, table):
        high = one.astype(bf16)
        low = (one - high.astype(np.float64)).astype(bf16)
        halves += [high, low]
    return np.stack(halves)


def mode_rows():
    position = np.arange(N)
    shift = (2.0 * np.sin(np.pi * position / N)) ** 2
    edges = (position == 0) | (position == N // 2)
    weight = np.where(edges, 1.0, 2.0) / N
    rows = np.zeros((8, N), np.float32)
    rows[0], rows[1] = shift, weight
    return rows


def split(value):
    high = value.astype(bf16)
    low = (value - high.astype(f32)).astype(bf16)
    return high, low


def dot(left, right):
    return jnp.dot(left, right, preferred_element_type=f32)


def dot3(left_high, left_low, right_high, right_low):
    return dot(left_high, right_high) + (dot(left_high, right_low) + dot(left_low, right_high))


def coords():
    k = lax.axis_index("kpt")
    g = lax.axis_index("grid")
    return g // 32 * 2 + k, lax.rem(g // 2, 4), lax.rem(g // 8, 4), lax.rem(g, 2)


def device(x, y, z, c):
    return lax.rem(x, 2), ((x // 2 * 4 + z) * 4 + y) * 2 + c


def for_each_peer(act):
    x, y, z, c = coords()
    across = []
    for step in (1, 3, 2, 0):
        tx = lax.rem(x + step, 4)
        for flip in range(2):
            across.append((step, lax.rem(tx, 2), tx // 2 * 32 + lax.rem(c + flip, 2)))

    def block(dy, dz, chosen):
        base = [lax.rem(z + dz + dx, 4) * 8 + lax.rem(y + dy + dx, 4) * 2 for dx in range(4)]
        for step, tk, part in chosen:
            act(tk, base[step] + part)

    def one(index, carry):
        block(lax.rem(index, 4), index // 4, across)
        return carry

    lax.fori_loop(1, 16, one, 0)
    block(0, 0, across[:6] + across[7:])


def rows_of(index, count):
    return pl.ds(pl.multiple_of(index * count, count), count)


def kernel(
    orb, kw_in, occ_in, zb, lam, tab_in, row_in, out,
    kwv, occv, obuf, zbuf, lamv, to_ky, to_jx, from_jx, from_ky, rowv, B, R, W, Q, Zh, Zl, ZhT, ZlT, fac,
    density, Xh, Xl, Yh, Yl, half, fcat, acat,
    orb_sem, in_sem, tab_sem, send_sem, recv_sem, back_sem, got_sem, column_sem,
):
    k = lax.axis_index("kpt")
    g = lax.axis_index("grid")
    me = k * 64 + g
    x, y, z, c = coords()

    def signal(sem, steps):
        for dx, dy, dz, dc in steps:
            tk, tg = device(
                lax.rem(x + dx, 4), lax.rem(y + dy, 4), lax.rem(z + dz, 4), lax.rem(c + dc, 2)
            )
            pl.semaphore_signal(sem, inc=1, device_id={"kpt": tk, "grid": tg}, device_id_type=MESH)

    plane_steps = [(i % 4, i // 4, 0, 0) for i in range(1, 16)]
    column_steps = [(0, 0, i % 4, i // 4) for i in range(1, 8)]
    barrier = pltpu.get_barrier_semaphore()
    signal(barrier, plane_steps + column_steps)

    def orb_copy(plane):
        return pltpu.make_async_copy(orb.at[:, :, :, plane], obuf.at[plane], orb_sem.at[plane])

    ins = [
        pltpu.make_async_copy(row_in, rowv, in_sem.at[1]),
        pltpu.make_async_copy(lam, lamv, in_sem.at[2]),
        pltpu.make_async_copy(zb, zbuf, in_sem.at[3]),
    ]
    scalars = [
        pltpu.make_async_copy(kw_in, kwv, in_sem.at[4]),
        pltpu.make_async_copy(occ_in, occv, in_sem.at[5]),
    ]
    for one in scalars:
        one.start()

    def table_copies(lo, hi):
        sources = [tab_in.at[0], tab_in.at[1], tab_in.at[2], tab_in.at[3]]
        sources += [
            tab_in.at[part, :, e * LANES : (e + 1) * LANES] for e in range(2) for part in (0, 0, 1)
        ]
        sources += [tab_in.at[2], tab_in.at[3], tab_in.at[2]]
        targets = [to_ky.at[0], to_ky.at[1], to_jx.at[0], to_jx.at[1]]
        targets += [
            from_jx.at[e, :, i * LANES : (i + 1) * LANES] for e in range(2) for i in range(3)
        ]
        targets += [from_ky.at[i * N : (i + 1) * N] for i in range(3)]
        return [
            pltpu.make_async_copy(sources[i], targets[i], tab_sem.at[i]) for i in range(lo, hi)
        ]

    orb_copy(0).start()
    for one in table_copies(0, 4):
        one.start()
    for plane in range(1, PLANES):
        orb_copy(plane).start()
    for one in table_copies(4, 13) + ins:
        one.start()

    for one in scalars:
        one.wait()
    weight = [[(kwv[p] * occv[p, b]).astype(f32) * (1.0 / 64.0) for b in range(2)] for p in range(2)]

    def plane_spectrum(plane):
        orb_copy(plane).wait()
        slot = plane % 2
        for r in range(0, N, 32):
            total = None
            for p in range(2):
                for b in range(2):
                    re = obuf[plane, p, b, 0, r : r + 32, :].astype(f32)
                    im = obuf[plane, p, b, 1, r : r + 32, :].astype(f32)
                    term = weight[p][b] * (re * re + im * im)
                    total = term if total is None else total + term
            high, low = split(total)
            density[slot, 0, r : r + 32, :] = high
            density[slot, 1, r : r + 32, :] = low
        if plane == 0:
            for one in table_copies(0, 4):
                one.wait()
        high, low = split(dot3(density[slot, 0], density[slot, 1], to_ky[0], to_ky[1]))
        both = dot3(to_jx[0], to_jx[1], high, low)
        h, q = plane // QUAD, plane % QUAD
        for e in range(2):
            for u in range(2):
                B[h, e, pl.ds(q * 2 + u, LANES, stride=8), :] = both[
                    e * LANES : (e + 1) * LANES, u * LANES : (u + 1) * LANES
                ]

    def send_out(h, e):
        def act(tk, tg):
            pltpu.make_async_remote_copy(
                src_ref=B.at[h, e, rows_of(tk * 64 + tg, 8)],
                dst_ref=R.at[e, rows_of(me * 2 + h, 8)],
                send_sem=send_sem,
                recv_sem=recv_sem.at[e],
                device_id={"kpt": tk, "grid": tg},
                device_id_type=MESH,
            ).start()

        for_each_peer(act)
        R[e, rows_of(me * 2 + h, 8), :] = B[h, e, rows_of(me, 8), :]

    plane_spectrum(0)
    pl.semaphore_wait(barrier, 22)
    signal(column_sem, column_steps)
    plane_spectrum(1)
    plane_spectrum(2)
    plane_spectrum(3)
    pl.semaphore_wait(column_sem, 7)
    send_out(0, 0)
    send_out(0, 1)
    for plane in range(QUAD, PLANES):
        plane_spectrum(plane)
    send_out(1, 0)
    send_out(1, 1)

    for one in table_copies(4, 13) + ins:
        one.wait()
    for r in range(0, NZ, LANES):
        rows = zbuf[r : r + LANES, :]
        high, low = split(rows)
        Zh[r : r + LANES, :] = high
        Zl[r : r + LANES, :] = low
        turned = rows.T
        high, low = split(turned)
        ZhT[:, r : r + LANES] = high
        ZlT[:, r : r + LANES] = low
    shift_y, weight_y = rowv[0:1, :], rowv[1:2, :]
    lanes = lax.broadcasted_iota(jnp.int32, (1, N), 1)
    for e in range(2):
        mine = lanes == e * LANES + me
        shift_x = jnp.sum(jnp.where(mine, shift_y, 0.0), axis=1, keepdims=True)
        weight_x = jnp.sum(jnp.where(mine, weight_y, 0.0), axis=1, keepdims=True)
        for r in range(0, NZ, LANES):
            column = jnp.broadcast_to(lamv[0:1, r : r + LANES], (LANES, LANES)).T
            for u in range(2):
                cols = slice(u * LANES, (u + 1) * LANES)
                fac[e, r : r + LANES, cols] = (weight_y[:, cols] * weight_x) / (
                    column + (shift_y[:, cols] + shift_x)
                )

    upper = lax.broadcasted_iota(jnp.int32, (8, LANES), 0) < QUAD

    def solve(e):
        taken = R.at[e, pl.ds(0, (DEVICES - 1) * 16)]
        pltpu.make_async_copy(taken, taken, recv_sem.at[e]).wait()
        for u in range(2):
            cols = slice(u * LANES, (u + 1) * LANES)
            for r in range(0, NZ, LANES):
                first = R[e, pl.ds(r * 2 + u, LANES, stride=2), :]
                second = R[e, pl.ds(1024 + r * 2 + u, LANES, stride=2), :]
                high, low = split(first + second)
                Xh[r : r + LANES, cols] = high
                Xl[r : r + LANES, cols] = low
        for r in range(0, NZ, N):
            part = dot3(ZhT[r : r + N, :], ZlT[r : r + N, :], Xh[...], Xl[...])
            high, low = split(part * fac[e, r : r + N, :])
            Yh[r : r + N, :] = high
            Yl[r : r + N, :] = low
        for r in range(0, NZ, N):
            part = dot3(Zh[r : r + N, :], Zl[r : r + N, :], Yh[...], Yl[...])
            for row in range(0, N, 8):
                first = part[row : row + 8, :LANES]
                second = part[row : row + 8, LANES:]
                at = slice(r + row, r + row + 8)
                W[e, 0, at, :] = jnp.where(upper, first, pltpu.roll(second, QUAD, 0))
                W[e, 1, at, :] = jnp.where(upper, pltpu.roll(first, QUAD, 0), second)

    def send_back(e, h):
        def act(tk, tg):
            pltpu.make_async_remote_copy(
                src_ref=W.at[e, h, rows_of(tg, 8)],
                dst_ref=Q.at[e, h, rows_of(me, 8)],
                send_sem=back_sem,
                recv_sem=got_sem.at[e + h * e],
                device_id={"kpt": tk, "grid": tg},
                device_id_type=MESH,
            ).start()

        for_each_peer(act)
        Q[e, h, rows_of(me, 8), :] = W[e, h, rows_of(g, 8), :]

    solve(0)
    send_back(0, 0)
    send_back(0, 1)
    solve(1)
    send_back(1, 0)
    send_back(1, 1)

    def half_done(e, plane):
        h, q = plane // QUAD, plane % QUAD
        parts = [Q[e, h, pl.ds(u * QUAD + q, LANES, stride=8), :] for u in range(2)]
        high, low = split(jnp.concatenate(parts, axis=1))
        slot = plane % 2
        fcat[slot, 0:LANES, :] = high
        fcat[slot, LANES : 2 * LANES, :] = low
        fcat[slot, 2 * LANES : 3 * LANES, :] = high
        return dot(from_jx[e], fcat[slot])

    def arrived(taken, sem):
        pltpu.make_async_copy(taken, taken, sem).wait()

    arrived(Q.at[0, :, pl.ds(0, (DEVICES - 1) * 8)], got_sem.at[0])
    for plane in range(PLANES):
        half[plane] = half_done(0, plane)
    for h in range(2):
        arrived(Q.at[1, h, pl.ds(0, (DEVICES - 1) * 8)], got_sem.at[1 + h])
        for plane in range(h * QUAD, (h + 1) * QUAD):
            high, low = split(half[plane] + half_done(1, plane))
            at = slice(plane % QUAD * N, (plane % QUAD + 1) * N)
            acat[at, 0:N] = high
            acat[at, N : 2 * N] = high
            acat[at, 2 * N : 3 * N] = low
        out[h * QUAD : (h + 1) * QUAD] = dot(acat[...], from_ky[...]).reshape(QUAD, N, N)

    arrived(R.at[:, pl.ds(0, (DEVICES - 1) * 16)], send_sem)
    arrived(Q.at[:, :, pl.ds(0, (DEVICES - 1) * 8)], back_sem)


def on_device(orbitals, kweights, occupations, z_basis, z_eigen):
    hbm = pl.BlockSpec(memory_space=pltpu.HBM)
    vmem = pltpu.VMEM
    dma = pltpu.SemaphoreType.DMA
    return pl.pallas_call(
        kernel,
        out_shape=jax.ShapeDtypeStruct((PLANES, N, N), f32),
        in_specs=[hbm] * 7,
        out_specs=pl.BlockSpec(memory_space=vmem),
        scratch_shapes=[
            pltpu.SMEM((2,), jnp.int32),
            pltpu.SMEM((2, 2), jnp.int32),
            vmem((PLANES, 2, 2, 2, N, N), bf16),
            vmem((NZ, NZ), f32),
            vmem((1, NZ), f32),
            vmem((2, N, N), bf16),
            vmem((2, N, N), bf16),
            vmem((2, N, 3 * LANES), bf16),
            vmem((3 * N, N), bf16),
            vmem((8, N), f32),
            vmem((2, 2, 1024, LANES), f32),
            vmem((2, 2048, LANES), f32),
            vmem((2, 2, 512, LANES), f32),
            vmem((2, 2, 1024, LANES), f32),
            vmem((NZ, NZ), bf16),
            vmem((NZ, NZ), bf16),
            vmem((NZ, NZ), bf16),
            vmem((NZ, NZ), bf16),
            vmem((2, NZ, N), f32),
            vmem((2, 2, N, N), bf16),
            vmem((NZ, N), bf16),
            vmem((NZ, N), bf16),
            vmem((NZ, N), bf16),
            vmem((NZ, N), bf16),
            vmem((PLANES, N, N), f32),
            vmem((2, 3 * LANES, N), bf16),
            vmem((QUAD * N, 3 * N), bf16),
            dma((PLANES,)),
            dma((6,)),
            dma((13,)),
            dma,
            dma((2,)),
            dma,
            dma((3,)),
            pltpu.SemaphoreType.REGULAR,
        ],
        compiler_params=pltpu.CompilerParams(
            collective_id=0, has_side_effects=True, vmem_limit_bytes=48 << 20
        ),
    )(*(pltpu.with_memory_space_constraint(one, pltpu.HBM) for one in (
        orbitals, kweights, occupations, z_basis, z_eigen.reshape(1, NZ),
        jnp.asarray(tables()), jnp.asarray(mode_rows()),
    )))


def solution(mesh):
    return jax.shard_map(
        on_device,
        mesh=mesh,
        in_specs=(P("kpt", None, None, "grid", None, None), P("kpt"), P("kpt", None), P(), P()),
        out_specs=P("grid", None, None),
        check_vma=False,
    )
```

```python
import functools

import jax
import jax.numpy as jnp
import numpy as np
from jax import lax
from jax.experimental import pallas as pl
from jax.experimental.pallas import tpu as pltpu
from jax.sharding import PartitionSpec as P

MESH = pl.DeviceIdType.MESH
f32 = jnp.float32
bf16 = jnp.bfloat16
N = 256
NZ = 512
LANES = 128
DEVICES = 128
PLANES = 8
QUAD = 4


def real_table():
    position = np.arange(N)
    angles = (position[:, None] * position[None, :] % N) * (2.0 * np.pi / N)
    return np.where(position[:, None] <= N // 2, np.cos(angles), np.sin(angles))


def tables():
    table = real_table()
    halves = []
    for one in (table.T, table):
        high = one.astype(bf16)
        low = (one - high.astype(np.float64)).astype(bf16)
        halves += [high, low]
    return np.stack(halves)


def mode_rows():
    position = np.arange(N)
    shift = (2.0 * np.sin(np.pi * position / N)) ** 2
    edges = (position == 0) | (position == N // 2)
    weight = np.where(edges, 1.0, 2.0) / N
    rows = np.zeros((8, N), np.float32)
    rows[0], rows[1] = shift, weight
    return rows


def split(value):
    high = value.astype(bf16)
    low = (value - high.astype(f32)).astype(bf16)
    return high, low


def dot(left, right):
    return jnp.dot(left, right, preferred_element_type=f32)


def dot3(left_high, left_low, right_high, right_low):
    return dot(left_high, right_high) + (dot(left_high, right_low) + dot(left_low, right_high))


def coords():
    k = lax.axis_index("kpt")
    g = lax.axis_index("grid")
    return g // 32 * 2 + k, lax.rem(g // 2, 4), lax.rem(g // 8, 4), lax.rem(g, 2)


def device(x, y, z, c):
    return lax.rem(x, 2), ((x // 2 * 4 + z) * 4 + y) * 2 + c


def for_each_peer(act):
    x, y, z, c = coords()
    across = []
    for step in (1, 3, 2, 0):
        tx = lax.rem(x + step, 4)
        for flip in range(2):
            across.append((lax.rem(tx, 2), tx // 2 * 32 + lax.rem(c + flip, 2)))

    def block(dy, dz, chosen):
        base = lax.rem(z + dz, 4) * 8 + lax.rem(y + dy, 4) * 2
        for tk, part in chosen:
            act(tk, base + part)

    def one(index, carry):
        block(lax.rem(index, 4), index // 4, across)
        return carry

    lax.fori_loop(1, 16, one, 0)
    block(0, 0, across[:6] + across[7:])


def rows_of(index, count):
    return pl.ds(pl.multiple_of(index * count, count), count)


def kernel(
    orb, kw_in, occ_in, zb, lam, tab_in, row_in, out,
    kwv, occv, obuf, zbuf, lamv, to_ky, to_jx, from_jx, from_ky, rowv, B, R, W, Q, Zh, Zl, ZhT, ZlT, fac,
    density, Xh, Xl, Yh, Yl, half, fcat, acat,
    orb_sem, in_sem, tab_sem, send_sem, recv_sem, back_sem, got_sem, column_sem,
):
    k = lax.axis_index("kpt")
    g = lax.axis_index("grid")
    me = k * 64 + g
    x, y, z, c = coords()

    def signal(sem, steps):
        for dx, dy, dz, dc in steps:
            tk, tg = device(
                lax.rem(x + dx, 4), lax.rem(y + dy, 4), lax.rem(z + dz, 4), lax.rem(c + dc, 2)
            )
            pl.semaphore_signal(sem, inc=1, device_id={"kpt": tk, "grid": tg}, device_id_type=MESH)

    plane_steps = [(i % 4, i // 4, 0, 0) for i in range(1, 16)]
    column_steps = [(0, 0, i % 4, i // 4) for i in range(1, 8)]
    barrier = pltpu.get_barrier_semaphore()
    signal(barrier, plane_steps + column_steps)

    def orb_copy(plane):
        return pltpu.make_async_copy(orb.at[:, :, :, plane], obuf.at[plane], orb_sem.at[plane])

    ins = [
        pltpu.make_async_copy(row_in, rowv, in_sem.at[1]),
        pltpu.make_async_copy(lam, lamv, in_sem.at[2]),
        pltpu.make_async_copy(zb, zbuf, in_sem.at[3]),
    ]
    scalars = [
        pltpu.make_async_copy(kw_in, kwv, in_sem.at[4]),
        pltpu.make_async_copy(occ_in, occv, in_sem.at[5]),
    ]
    for one in scalars:
        one.start()

    def table_copies(lo, hi):
        sources = [tab_in.at[0], tab_in.at[1], tab_in.at[2], tab_in.at[3]]
        sources += [
            tab_in.at[part, :, e * LANES : (e + 1) * LANES] for e in range(2) for part in (0, 0, 1)
        ]
        sources += [tab_in.at[2], tab_in.at[3], tab_in.at[2]]
        targets = [to_ky.at[0], to_ky.at[1], to_jx.at[0], to_jx.at[1]]
        targets += [
            from_jx.at[e, :, i * LANES : (i + 1) * LANES] for e in range(2) for i in range(3)
        ]
        targets += [from_ky.at[i * N : (i + 1) * N] for i in range(3)]
        return [
            pltpu.make_async_copy(sources[i], targets[i], tab_sem.at[i]) for i in range(lo, hi)
        ]

    orb_copy(0).start()
    for one in table_copies(0, 4):
        one.start()
    for plane in range(1, PLANES):
        orb_copy(plane).start()
    for one in table_copies(4, 13) + ins:
        one.start()

    for one in scalars:
        one.wait()
    weight = [[(kwv[p] * occv[p, b]).astype(f32) * (1.0 / 64.0) for b in range(2)] for p in range(2)]

    def plane_spectrum(plane):
        orb_copy(plane).wait()
        slot = plane % 2
        for r in range(0, N, 32):
            total = None
            for p in range(2):
                for b in range(2):
                    re = obuf[plane, p, b, 0, r : r + 32, :].astype(f32)
                    im = obuf[plane, p, b, 1, r : r + 32, :].astype(f32)
                    term = weight[p][b] * (re * re + im * im)
                    total = term if total is None else total + term
            high, low = split(total)
            density[slot, 0, r : r + 32, :] = high
            density[slot, 1, r : r + 32, :] = low
        if plane == 0:
            for one in table_copies(0, 4):
                one.wait()
        high, low = split(dot3(density[slot, 0], density[slot, 1], to_ky[0], to_ky[1]))
        both = dot3(to_jx[0], to_jx[1], high, low)
        h, q = plane // QUAD, plane % QUAD
        for e in range(2):
            for u in range(2):
                B[h, e, pl.ds(q * 2 + u, LANES, stride=8), :] = both[
                    e * LANES : (e + 1) * LANES, u * LANES : (u + 1) * LANES
                ]

    def send_out(h, e):
        def act(tk, tg):
            pltpu.make_async_remote_copy(
                src_ref=B.at[h, e, rows_of(tk * 64 + tg, 8)],
                dst_ref=R.at[e, rows_of(me * 2 + h, 8)],
                send_sem=send_sem,
                recv_sem=recv_sem.at[e],
                device_id={"kpt": tk, "grid": tg},
                device_id_type=MESH,
            ).start()

        for_each_peer(act)
        R[e, rows_of(me * 2 + h, 8), :] = B[h, e, rows_of(me, 8), :]

    plane_spectrum(0)
    pl.semaphore_wait(barrier, 22)
    signal(column_sem, column_steps)
    plane_spectrum(1)
    plane_spectrum(2)
    plane_spectrum(3)
    pl.semaphore_wait(column_sem, 7)
    send_out(0, 0)
    send_out(0, 1)
    for plane in range(QUAD, PLANES):
        plane_spectrum(plane)
    send_out(1, 0)
    send_out(1, 1)

    for one in table_copies(4, 13) + ins:
        one.wait()
    for r in range(0, NZ, LANES):
        rows = zbuf[r : r + LANES, :]
        high, low = split(rows)
        Zh[r : r + LANES, :] = high
        Zl[r : r + LANES, :] = low
        turned = rows.T
        high, low = split(turned)
        ZhT[:, r : r + LANES] = high
        ZlT[:, r : r + LANES] = low
    shift_y, weight_y = rowv[0:1, :], rowv[1:2, :]
    lanes = lax.broadcasted_iota(jnp.int32, (1, N), 1)
    for e in range(2):
        mine = lanes == e * LANES + me
        shift_x = jnp.sum(jnp.where(mine, shift_y, 0.0), axis=1, keepdims=True)
        weight_x = jnp.sum(jnp.where(mine, weight_y, 0.0), axis=1, keepdims=True)
        for r in range(0, NZ, LANES):
            column = jnp.broadcast_to(lamv[0:1, r : r + LANES], (LANES, LANES)).T
            for u in range(2):
                cols = slice(u * LANES, (u + 1) * LANES)
                fac[e, r : r + LANES, cols] = (weight_y[:, cols] * weight_x) / (
                    column + (shift_y[:, cols] + shift_x)
                )

    upper = lax.broadcasted_iota(jnp.int32, (8, LANES), 0) < QUAD

    def solve(e):
        taken = R.at[e, pl.ds(0, (DEVICES - 1) * 16)]
        pltpu.make_async_copy(taken, taken, recv_sem.at[e]).wait()
        for u in range(2):
            cols = slice(u * LANES, (u + 1) * LANES)
            for r in range(0, NZ, LANES):
                first = R[e, pl.ds(r * 2 + u, LANES, stride=2), :]
                second = R[e, pl.ds(1024 + r * 2 + u, LANES, stride=2), :]
                high, low = split(first + second)
                Xh[r : r + LANES, cols] = high
                Xl[r : r + LANES, cols] = low
        for r in range(0, NZ, N):
            part = dot3(ZhT[r : r + N, :], ZlT[r : r + N, :], Xh[...], Xl[...])
            high, low = split(part * fac[e, r : r + N, :])
            Yh[r : r + N, :] = high
            Yl[r : r + N, :] = low
        for r in range(0, NZ, N):
            part = dot3(Zh[r : r + N, :], Zl[r : r + N, :], Yh[...], Yl[...])
            for row in range(0, N, 8):
                first = part[row : row + 8, :LANES]
                second = part[row : row + 8, LANES:]
                at = slice(r + row, r + row + 8)
                W[e, 0, at, :] = jnp.where(upper, first, pltpu.roll(second, QUAD, 0))
                W[e, 1, at, :] = jnp.where(upper, pltpu.roll(first, QUAD, 0), second)

    def send_back(e, h):
        def act(tk, tg):
            pltpu.make_async_remote_copy(
                src_ref=W.at[e, h, rows_of(tg, 8)],
                dst_ref=Q.at[e, h, rows_of(me, 8)],
                send_sem=back_sem,
                recv_sem=got_sem.at[e + h * e],
                device_id={"kpt": tk, "grid": tg},
                device_id_type=MESH,
            ).start()

        for_each_peer(act)
        Q[e, h, rows_of(me, 8), :] = W[e, h, rows_of(g, 8), :]

    solve(0)
    send_back(0, 0)
    send_back(0, 1)
    solve(1)
    send_back(1, 0)
    send_back(1, 1)

    def half_done(e, plane):
        h, q = plane // QUAD, plane % QUAD
        parts = [Q[e, h, pl.ds(u * QUAD + q, LANES, stride=8), :] for u in range(2)]
        high, low = split(jnp.concatenate(parts, axis=1))
        slot = plane % 2
        fcat[slot, 0:LANES, :] = high
        fcat[slot, LANES : 2 * LANES, :] = low
        fcat[slot, 2 * LANES : 3 * LANES, :] = high
        return dot(from_jx[e], fcat[slot])

    def arrived(taken, sem):
        pltpu.make_async_copy(taken, taken, sem).wait()

    arrived(Q.at[0, :, pl.ds(0, (DEVICES - 1) * 8)], got_sem.at[0])
    for plane in range(PLANES):
        half[plane] = half_done(0, plane)
    for h in range(2):
        arrived(Q.at[1, h, pl.ds(0, (DEVICES - 1) * 8)], got_sem.at[1 + h])
        for plane in range(h * QUAD, (h + 1) * QUAD):
            high, low = split(half[plane] + half_done(1, plane))
            at = slice(plane % QUAD * N, (plane % QUAD + 1) * N)
            acat[at, 0:N] = high
            acat[at, N : 2 * N] = high
            acat[at, 2 * N : 3 * N] = low
        out[h * QUAD : (h + 1) * QUAD] = dot(acat[...], from_ky[...]).reshape(QUAD, N, N)

    arrived(R.at[:, pl.ds(0, (DEVICES - 1) * 16)], send_sem)
    arrived(Q.at[:, :, pl.ds(0, (DEVICES - 1) * 8)], back_sem)


def on_device(orbitals, kweights, occupations, z_basis, z_eigen):
    hbm = pl.BlockSpec(memory_space=pltpu.HBM)
    vmem = pltpu.VMEM
    dma = pltpu.SemaphoreType.DMA
    return pl.pallas_call(
        kernel,
        out_shape=jax.ShapeDtypeStruct((PLANES, N, N), f32),
        in_specs=[hbm] * 7,
        out_specs=pl.BlockSpec(memory_space=vmem),
        scratch_shapes=[
            pltpu.SMEM((2,), jnp.int32),
            pltpu.SMEM((2, 2), jnp.int32),
            vmem((PLANES, 2, 2, 2, N, N), bf16),
            vmem((NZ, NZ), f32),
            vmem((1, NZ), f32),
            vmem((2, N, N), bf16),
            vmem((2, N, N), bf16),
            vmem((2, N, 3 * LANES), bf16),
            vmem((3 * N, N), bf16),
            vmem((8, N), f32),
            vmem((2, 2, 1024, LANES), f32),
            vmem((2, 2048, LANES), f32),
            vmem((2, 2, 512, LANES), f32),
            vmem((2, 2, 1024, LANES), f32),
            vmem((NZ, NZ), bf16),
            vmem((NZ, NZ), bf16),
            vmem((NZ, NZ), bf16),
            vmem((NZ, NZ), bf16),
            vmem((2, NZ, N), f32),
            vmem((2, 2, N, N), bf16),
            vmem((NZ, N), bf16),
            vmem((NZ, N), bf16),
            vmem((NZ, N), bf16),
            vmem((NZ, N), bf16),
            vmem((PLANES, N, N), f32),
            vmem((2, 3 * LANES, N), bf16),
            vmem((QUAD * N, 3 * N), bf16),
            dma((PLANES,)),
            dma((6,)),
            dma((13,)),
            dma,
            dma((2,)),
            dma,
            dma((3,)),
            pltpu.SemaphoreType.REGULAR,
        ],
        compiler_params=pltpu.CompilerParams(
            collective_id=0, has_side_effects=True, vmem_limit_bytes=48 << 20
        ),
    )(*(pltpu.with_memory_space_constraint(one, pltpu.HBM) for one in (
        orbitals, kweights, occupations, z_basis, z_eigen.reshape(1, NZ),
        jnp.asarray(tables()), jnp.asarray(mode_rows()),
    )))


def solution(mesh):
    return jax.shard_map(
        on_device,
        mesh=mesh,
        in_specs=(P("kpt", None, None, "grid", None, None), P("kpt"), P("kpt", None), P(), P()),
        out_specs=P("grid", None, None),
        check_vma=False,
    )
```
